32 devices in a mesh: dp: 4 (over z), fsdp: 8 (over y, x, core).
Axes of the slice: x: 2, y: 2, z: 4, core: 2. Of those that a mesh axis runs over, the one named last changes fastest.
Arguments:
- inputs: bfloat16 [2, 2048, 2048], P(None, ('dp', 'fsdp')), may hold values from -6 to 6
- seq_len: int32 [2, 32], P(None, ('dp', 'fsdp')), may hold values from 32 to 64, as said below
- gain_one: bfloat16 [2048], P(('dp', 'fsdp')), may hold values from 0.5 to 1.5
- w_query: bfloat16 [2048, 2048], P(('dp', 'fsdp')), may hold values from -0.125 to 0.125
- w_key: bfloat16 [2048, 128], P(('dp', 'fsdp')), may hold values from -0.125 to 0.125
- w_value: bfloat16 [2048, 128], P(('dp', 'fsdp')), may hold values from -0.125 to 0.125
- w_output: bfloat16 [2048, 2048], P(('dp', 'fsdp')), may hold values from -1 to 1
- gain_two: bfloat16 [2048], P(('dp', 'fsdp')), may hold values from 0.5 to 1.5
- w_gate: bfloat16 [2048, 5632], P(('dp', 'fsdp')), may hold values from -0.125 to 0.125
- w_up: bfloat16 [2048, 5632], P(('dp', 'fsdp')), may hold values from -0.125 to 0.125
- w_down: bfloat16 [5632, 2048], P(('dp', 'fsdp')), may hold values from -0.078125 to 0.078125
- d_out: bfloat16 [2, 2048, 2048], P(None, ('dp', 'fsdp')), may hold values from -6 to 6
- d_key: bfloat16 [2, 2048, 128], P(None, ('dp', 'fsdp')), may hold values from -6 to 6
- d_value: bfloat16 [2, 2048, 128], P(None, ('dp', 'fsdp')), may hold values from -6 to 6
Outputs:
- output: bfloat16 [2, 2048, 2048], P(None, ('dp', 'fsdp'))
- key_out: bfloat16 [2, 2048, 128], P(None, ('dp', 'fsdp'))
- value_out: bfloat16 [2, 2048, 128], P(None, ('dp', 'fsdp'))
- d_inputs: bfloat16 [2, 2048, 2048], P(None, ('dp', 'fsdp'))
- grad_gain_one: float32 [2048], P(('dp', 'fsdp'))
- grad_query: float32 [2048, 2048], P(('dp', 'fsdp'))
- grad_key: float32 [2048, 128], P(('dp', 'fsdp'))
- grad_value: float32 [2048, 128], P(('dp', 'fsdp'))
- grad_output: float32 [2048, 2048], P(('dp', 'fsdp'))
- grad_gain_two: float32 [2048], P(('dp', 'fsdp'))
- grad_gate: float32 [2048, 5632], P(('dp', 'fsdp'))
- grad_up: float32 [2048, 5632], P(('dp', 'fsdp'))
- grad_down: float32 [5632, 2048], P(('dp', 'fsdp'))
The draws below stay inside these ranges and needn't reach their ends.
Inputs may be any that keep to these rules, and one draw needn't show every extreme that they name: `seq_len`: each entry is 64 (one sequence fills the buffer) or 64/2 (two sequences of 32).
All inputs are finite; a program needn't handle non-finite values.
Results may differ from the reference program's by a relative error of at most 0.013.
Values may be sent and summed in bfloat16 or wider, within the bound.
A program may use at most 384 MiB of HBM per device.

```python
import math
import jax
import jax.numpy as jnp
from jax import lax

D = 2048
HD = 128
FF = 5632
CAP = 64
MB = 2
HOLDERS = 32
ROWS = 2048


def draw_seq_len(key, part):
    half = CAP // 2
    picked = jax.random.randint(key, (MB, HOLDERS), 0, 2)
    values = half + picked * half
    values = values.at[0, 0].set(CAP).at[0, 1].set(half)
    return values.astype(jnp.int32)


def block_scale(key, dims, pieces, low, top_value):
    factor_of = 1.0
    for axis_at, shards_of in pieces:
        heights = jax.random.uniform(jax.random.fold_in(jax.random.fold_in(key, 6), axis_at), (shards_of,), jnp.float32, low / len(pieces), top_value / len(pieces))
        factor_of = factor_of * jnp.repeat(jnp.exp(heights), dims[axis_at] // shards_of).reshape((-1,) + (1,) * (len(dims) - 1 - axis_at))
    return factor_of


def noise(key, dims, scale, most, shards=(), held_as=jnp.bfloat16):
    entries = jax.random.normal(key, dims, jnp.float32) * scale
    if len(shards) > 0:
        entries = block_scale(key, dims, shards, -0.22, 0.18) * entries
    return jnp.clip(entries, min=-most, max=most).astype(held_as)


def setup_inputs(seed: int = 0) -> dict:
    key_of = jax.random.split(jax.random.key(seed), 15)
    return {
        "inputs": noise(key_of[0], (MB, ROWS, D), 1.0, 6.0, ((1, 32),)),
        "seq_len": draw_seq_len(jax.random.fold_in(key_of[14], 71), 0),
        "gain_one": jnp.clip(1.0 + 0.1 * jax.random.normal(key_of[2], (D,), jnp.float32), 0.5, 1.5).astype(jnp.bfloat16),
        "w_query": noise(key_of[3], (D, D), D ** -0.5, 0.125, ((0, 32),)),
        "w_key": noise(key_of[4], (D, HD), D ** -0.5, 0.125, ((0, 32),)),
        "w_value": noise(key_of[5], (D, HD), D ** -0.5, 0.125, ((0, 32),)),
        "w_output": noise(key_of[6], (D, D), (D // 64) ** -0.5, 1.0, ((0, 32),)),
        "gain_two": jnp.clip(1.0 + 0.1 * jax.random.normal(key_of[7], (D,), jnp.float32), 0.5, 1.5).astype(jnp.bfloat16),
        "w_gate": noise(key_of[8], (D, FF), D ** -0.5, 0.125, ((0, 32),)),
        "w_up": noise(key_of[9], (D, FF), D ** -0.5, 0.125, ((0, 32),)),
        "w_down": noise(key_of[10], (FF, D), FF ** -0.5, 0.078125, ((0, 32),)),
        "d_out": noise(key_of[11], (MB, ROWS, D), 1.0, 6.0, ((1, 32),)),
        "d_key": noise(key_of[12], (MB, ROWS, HD), 1.0, 6.0, ((1, 32),)),
        "d_value": noise(key_of[13], (MB, ROWS, HD), 1.0, 6.0, ((1, 32),)),
    }


@jax.custom_vjp
def low(v):
    return lax.optimization_barrier(v.astype(jnp.bfloat16)).astype(jnp.float32)

@jax.custom_vjp
def low_back(v):
    return v

def low_keep(v):
    return (low(v), None)

def low_pass(kept, grad):
    return (grad,)

def back_keep(v):
    return (v, None)

def back_low(kept, grad):
    return (low(grad),)
low.defvjp(low_keep, low_pass)
low_back.defvjp(back_keep, back_low)
highest = lax.Precision.HIGHEST
group_buffers = 16

def rope_tables(first_len, count):
    place = jnp.arange(count, dtype=jnp.int32)
    second = (place >= first_len).astype(jnp.int32)
    offset = place - first_len * second
    half = HD // 2
    freq = jnp.exp(jnp.arange(half, dtype=jnp.float32) * (-2.0 * math.log(10000.0) / HD))
    angle = offset.astype(jnp.float32)[:, None] * freq[None, :]
    return (jnp.cos(angle), jnp.sin(angle), second)

def rotate(values, cosine, sine):
    shape = (values.shape[0],) + (1,) * (values.ndim - 2) + (cosine.shape[1],)
    cosine = cosine.reshape(shape)
    sine = sine.reshape(shape)
    half = values.shape[-1] // 2
    first = values[..., :half]
    last = values[..., half:]
    return jnp.concatenate([first * cosine - last * sine, last * cosine + first * sine], axis=-1)

def normalize(values):
    return values * lax.rsqrt(lax.optimization_barrier(jnp.mean(values * values, axis=-1, keepdims=True)) + 1e-05)

def attend(query, key, value, first_len):
    count = query.shape[0]
    cosine, sine, second = rope_tables(first_len, count)
    q_rot = low(rotate(low_back(query), cosine, sine))
    k_rot = low(rotate(low_back(key), cosine, sine))
    v_low = low(low_back(value))
    logits = low_back(jnp.einsum('qhd,kd->hqk', q_rot, k_rot, precision=highest) * HD ** (-0.5))
    place = jnp.arange(count, dtype=jnp.int32)
    allowed = (second[:, None] == second[None, :]) & (place[None, :] <= place[:, None])
    logits = jnp.where(allowed[None], logits, -1e+30)
    top = lax.optimization_barrier(jnp.max(logits, axis=-1, keepdims=True))
    expo = jnp.exp(logits - top)
    probs = expo / lax.optimization_barrier(jnp.sum(expo, axis=-1, keepdims=True))
    mixed = jnp.einsum('hqk,kd->qhd', low(probs), v_low, precision=highest)
    return (mixed.reshape(count, -1), k_rot, v_low)

def block(pair, weights):
    group, lens = pair
    gain_one, w_query, w_key, w_value, w_output, gain_two, w_gate, w_up, w_down = weights
    buffers, count, width = group.shape
    rows = group.reshape(buffers * count, width)
    act = low(normalize(rows) * gain_one)
    query = jnp.dot(act, w_query, precision=highest).reshape(buffers, count, width // HD, HD)
    key = jnp.dot(act, w_key, precision=highest).reshape(buffers, count, HD)
    value = jnp.dot(act, w_value, precision=highest).reshape(buffers, count, HD)
    mixed, k_rot, v_low = jax.vmap(attend)(query, key, value, lens)
    mixed = low(low_back(mixed.reshape(buffers * count, width)))
    branch = low_back(jnp.dot(mixed, w_output, precision=highest))
    hidden = rows + branch
    act_two = low(normalize(hidden) * gain_two)
    gate = low_back(jnp.dot(act_two, w_gate, precision=highest))
    up = low_back(jnp.dot(act_two, w_up, precision=highest))
    swish = low(gate * jax.nn.sigmoid(gate) * up)
    output = hidden + jnp.dot(swish, w_down, precision=highest)
    return (output.reshape(buffers, count, width), k_rot, v_low)

def forward(values, lens, weights):
    groups = values.reshape(-1, group_buffers, CAP, D)
    len_groups = lens.reshape(-1, group_buffers)

    def step(pair):
        return block(pair, weights)
    output, key_out, value_out = lax.map(jax.checkpoint(step), (groups, len_groups))
    return (output.reshape(MB, -1, D), key_out.reshape(MB, -1, HD), value_out.reshape(MB, -1, HD))

def reference(inputs, seq_len, gain_one, w_query, w_key, w_value, w_output, gain_two, w_gate, w_up, w_down, d_out, d_key, d_value):
    weights = tuple((item.astype(jnp.float32) for item in (gain_one, w_query, w_key, w_value, w_output, gain_two, w_gate, w_up, w_down)))
    lens = seq_len.reshape(-1).astype(jnp.int32)

    def whole(values, params):
        return forward(values, lens, params)
    results, pull = jax.vjp(whole, inputs.astype(jnp.float32), weights)
    grad_in, grads = pull((d_out.astype(jnp.float32), d_key.astype(jnp.float32), d_value.astype(jnp.float32)))
    output, key_out, value_out = results
    return (output.astype(jnp.bfloat16), key_out.astype(jnp.bfloat16), value_out.astype(jnp.bfloat16), grad_in.astype(jnp.bfloat16), grads[0], grads[1], grads[2], grads[3], grads[4], grads[5], grads[6], grads[7], grads[8])
```

```python
import math

import jax
import jax.numpy as jnp
from jax import lax
from jax.sharding import Mesh, PartitionSpec as P

HD = 128
EPS = 1e-05
BF = jnp.bfloat16
F32 = jnp.float32
AXES = ("zh", "zl", "y", "x", "c")
TP = ("zl", "x", "c")


def size(axis):
    return lax.axis_size(axis)


def swap(value, axis, k=1):
    count = math.prod(size(a) for a in axis) if isinstance(axis, tuple) else size(axis)
    return lax.ppermute(value, axis, [(i, i ^ k) for i in range(count)])


def pick(value, index):
    return lax.dynamic_index_in_dim(value, index, 0, keepdims=False)


def place(target, block, index):
    return lax.dynamic_update_slice(target, block[None], (index,) + (0,) * block.ndim)


def tp_index():
    return (lax.axis_index("zl") * 2 + lax.axis_index("x")) * 2 + lax.axis_index("c")


def gather_tp(v):
    h = v.shape[0] // 2
    vx = swap(v, "x")
    vz = swap(v, "zl")
    parts = [v, vx, vz, swap(vx[:h], "zl"), swap(vz[h:], "x")]
    return jnp.concatenate(parts + [swap(p, "c") for p in parts], axis=0)


def scatter_tp(p):
    rows = p.shape[0] // 8
    h = rows // 2
    p = p.reshape(2, 4, rows, p.shape[1])
    s = p[0] + swap(p[1].astype(BF), "c").astype(F32)
    top = s[:, :h]
    low = s[:, h:]
    got_top = swap(top[2:].astype(BF), "zl").astype(F32)
    got_low = swap(low[1::2].astype(BF), "x").astype(F32)
    out_top = top[0] + got_top[0] + swap((top[1] + got_top[1]).astype(BF), "x").astype(F32)
    out_low = low[0] + got_low[0] + swap((low[2] + got_low[1]).astype(BF), "zl").astype(F32)
    return jnp.concatenate([out_top, out_low], axis=0)


def exchange_tp(v):
    me = tp_index()
    out = jnp.zeros_like(v)
    for k in range(8):
        block = pick(v, me ^ k)
        if k:
            block = swap(block, TP, k)
        out = place(out, block, me ^ k)
    return out


def gather_dp(v):
    zs = size("zh")
    ys = size("y")
    mz = lax.axis_index("zh")
    my = lax.axis_index("y")
    out = jnp.zeros((zs, ys) + v.shape, v.dtype)
    for kz in range(zs):
        first = swap(v, "zh", kz) if kz else v
        for ky in range(ys):
            block = swap(first, "y", ky) if ky else first
            out = lax.dynamic_update_slice(
                out, block[None, None], (mz ^ kz, my ^ ky) + (0,) * v.ndim
            )
    return out


def scatter_dp(block_of):
    zs = size("zh")
    ys = size("y")
    mz = lax.axis_index("zh")
    my = lax.axis_index("y")
    sums = [block_of(mz ^ kz, my) for kz in range(zs)]
    for ky in range(1, ys):
        sent = [block_of(mz ^ kz, my ^ ky).astype(BF) for kz in range(zs)]
        for kz in range(zs - 1, -1, -1):
            sums[kz] = sums[kz] + swap(sent[kz], "y", ky).astype(F32)
    total = sums[0]
    for kz in range(1, zs):
        total = total + swap(sums[kz].astype(BF), "zh", kz).astype(F32)
    return total


def gather_all(v):
    blocks = v[None]
    order = jnp.zeros((1,), jnp.int32)
    stride = 1
    for axis in reversed(AXES):
        n = size(axis)
        me = lax.axis_index(axis)
        parts = [blocks] + [swap(blocks, axis, k) for k in range(1, n)]
        order = jnp.concatenate([order + stride * (me ^ k) for k in range(n)])
        blocks = jnp.concatenate(parts, axis=0)
        stride *= n
    hot = (jnp.arange(stride)[:, None] == order[None, :]).astype(F32)
    flat = blocks.reshape(stride, -1).astype(F32)
    return jnp.dot(hot, flat, precision=lax.Precision.HIGHEST).reshape(blocks.shape)


def scatter_all(v):
    value = v.reshape(tuple(size(a) for a in AXES) + (-1,))
    for axis in AXES:
        me = lax.axis_index(axis)
        total = pick(value, me)
        for k in range(1, size(axis)):
            total = total + swap(pick(value, me ^ k), axis, k)
        value = total
    return value


def rotate(values, cosine, sine):
    half = HD // 2
    first = values[..., :half]
    last = values[..., half:]
    return jnp.concatenate([first * cosine - last * sine, last * cosine + first * sine], axis=-1)


def inverse_norm(values):
    return lax.rsqrt(jnp.mean(values * values, axis=-1, keepdims=True) + EPS)


def dot(left, right):
    return jnp.dot(left, right, preferred_element_type=F32)


def dot_t(left, right):
    return lax.dot_general(left, right, (((1,), (1,)), ((), ())), preferred_element_type=F32)


def t_dot(left, right):
    return lax.dot_general(left, right, (((0,), (0,)), ((), ())), preferred_element_type=F32)


def batched(eq, left, right):
    return jnp.einsum(eq, left, right, preferred_element_type=F32)


def per_device(
    inputs,
    seq_len,
    gain_one,
    w_query,
    w_key,
    w_value,
    w_output,
    gain_two,
    w_gate,
    w_up,
    w_down,
    d_out,
    d_key,
    d_value,
):
    zs, ys = size("zh"), size("y")
    mb, cap, width = inputs.shape
    rows_own = mb * cap
    depth = w_query.shape[0]
    heads = width // HD
    own_heads = heads // 8
    own_width = own_heads * HD
    wide = w_gate.shape[1] // 8
    part = w_down.shape[0]
    paired = zs == 2 and ys == 2 and depth * 2 == HD and own_heads == 2
    zl, x, c = (lax.axis_index(a) for a in TP)

    x_own = inputs.reshape(rows_own, width)
    x_all = gather_tp(x_own)
    lens = seq_len.astype(jnp.int32).reshape(mb, 1)
    lens_parts = [lens] + [swap(lens, TP, k) for k in (2, 4, 6, 1, 3, 5, 7)]
    lens_all = jnp.concatenate(lens_parts, axis=0)
    gains = gather_all(jnp.stack([gain_one, gain_two]))
    gains = jnp.swapaxes(gains, 0, 1).reshape(2, 1, width)
    gain_a, gain_b = gains[0], gains[1]

    if paired:
        q_cols = w_query.reshape(depth, 2, 2, 2, 2, HD).transpose(2, 4, 1, 0, 3, 5)
    else:
        q_cols = w_query.reshape(depth, 2, 2, 2, own_heads, HD).transpose(1, 2, 3, 0, 4, 5)
    q_cols = q_cols.reshape(8, depth, own_width)
    kv_cols = jnp.broadcast_to(jnp.concatenate([w_key, w_value], axis=1)[None], (8, depth, 2 * HD))
    qkv = exchange_tp(jnp.concatenate([q_cols, kv_cols], axis=2))
    qkv_width = own_width + 2 * HD

    def to_rows(gathered, columns):
        g = gathered.reshape(zs, ys, 2, 2, 2, depth, columns)
        return g.transpose(0, 2, 1, 3, 4, 5, 6).reshape(width, columns)

    w_qkv = to_rows(gather_dp(qkv), qkv_width)
    if paired:
        wo = gather_dp(w_output)
        wo_mine = pick(wo, c)
        wo_other = swap(pick(wo, 1 - c), "c")
        w_o = jnp.stack(
            [jnp.where(c == 0, wo_mine, wo_other), jnp.where(c == 0, wo_other, wo_mine)], axis=1
        ).reshape(own_width, width)
    else:
        w_o_full = lax.all_gather(w_output, AXES, axis=0, tiled=True)
        w_o = lax.dynamic_slice_in_dim(w_o_full, tp_index() * own_width, own_width, 0)

    def split_columns(w):
        w = w.reshape(depth, zs, 2, ys, 2, 2, part).transpose(2, 4, 5, 0, 1, 3, 6)
        return w.reshape(8, depth, wide)

    wg = to_rows(gather_dp(exchange_tp(split_columns(w_gate))), wide)
    wu = to_rows(gather_dp(exchange_tp(split_columns(w_up))), wide)
    wd = gather_dp(w_down).reshape(wide, width)
    do_own = d_out.reshape(rows_own, width)
    do_all = gather_tp(do_own)

    rows = x_all.shape[0]
    buffers = rows // cap
    xf = x_all.astype(F32)
    act = (xf * inverse_norm(xf) * gain_a).astype(BF)
    qkv_out = dot(act, w_qkv)
    place_at = jnp.arange(cap, dtype=jnp.int32)[None, :]
    second = (place_at >= lens_all).astype(jnp.int32)
    offset = (place_at - lens_all * second).astype(F32)
    freq = jnp.exp(jnp.arange(HD // 2, dtype=F32) * (-2.0 * math.log(10000.0) / HD))
    angle = offset[:, :, None] * freq[None, None, :]
    cosine, sine = jnp.cos(angle), jnp.sin(angle)
    cos_h, sin_h = cosine[:, None], sine[:, None]
    query = qkv_out[:, :own_width].reshape(buffers, cap, own_heads, HD).transpose(0, 2, 1, 3)
    key = qkv_out[:, own_width : own_width + HD].reshape(buffers, cap, HD)
    value = qkv_out[:, own_width + HD :].reshape(buffers, cap, HD)
    q_rot = rotate(query, cos_h, sin_h).astype(BF)
    k_rot = rotate(key, cosine, sine).astype(BF)
    v_low = value.astype(BF)
    allowed = (second[:, :, None] == second[:, None, :]) & (
        place_at[0][None, None, :] <= place_at[0][None, :, None]
    )
    scale = HD ** (-0.5)
    logits = batched("bhqd,bkd->bhqk", q_rot, k_rot) * scale
    logits = jnp.where(allowed[:, None], logits, -1e30)
    top = jnp.max(logits, axis=-1, keepdims=True)
    expo = jnp.exp(logits - top)
    total = jnp.sum(expo, axis=-1, keepdims=True)
    probs = expo / total
    probs_low = probs.astype(BF)
    mixed = batched("bhqk,bkd->bhqd", probs_low, v_low).astype(BF)
    mixed = mixed.transpose(0, 2, 1, 3).reshape(rows, own_width)
    branch = scatter_tp(dot(mixed, w_o))
    hidden = x_own.astype(F32) + branch
    inverse_two = inverse_norm(hidden)
    normed_two = hidden * inverse_two
    act_two = gather_tp((normed_two * gain_b).astype(BF))

    gate = dot(act_two, wg)
    up = dot(act_two, wu)
    sigma = jax.nn.sigmoid(gate)
    swish = (gate * sigma * up).astype(BF)
    d_swish = dot_t(do_all, wd)
    d_gate = (d_swish * up * sigma * (1.0 + gate * (1.0 - sigma))).astype(BF)
    d_up = (d_swish * gate * sigma).astype(BF)
    d_act_two = scatter_tp(dot_t(d_gate, wg) + dot_t(d_up, wu))
    output = (hidden + scatter_tp(dot(swish, wd))).astype(BF)

    scaled = d_act_two * gain_b
    d_hidden = do_own.astype(F32) + inverse_two * (
        scaled - normed_two * jnp.mean(scaled * normed_two, axis=-1, keepdims=True)
    )
    grad_gain_two = scatter_all(jnp.sum(d_act_two * normed_two, axis=0))
    d_branch = gather_tp(d_hidden.astype(BF))

    def rows_of(g):
        g = g.reshape(zs, 2, ys, 2, 2, depth, g.shape[-1])

        def block_of(iz, iy):
            b = lax.dynamic_slice(
                g, (iz, 0, iy, 0, 0, 0, 0), (1, 2, 1, 2, 2) + g.shape[5:]
            )
            return b.reshape((8,) + g.shape[5:])

        return block_of

    def blocks_of(g):
        def block_of(iz, iy):
            b = lax.dynamic_slice(g, (iz, iy) + (0,) * (g.ndim - 2), (1, 1) + g.shape[2:])
            return b.reshape(g.shape[2:])

        return block_of

    def join_columns(g):
        g = exchange_tp(scatter_dp(rows_of(g)).astype(BF))
        g = g.reshape(2, 2, 2, depth, zs, ys, part).transpose(3, 4, 0, 5, 1, 2, 6)
        return g.reshape(depth, 8 * wide).astype(F32)

    grad_down = scatter_dp(blocks_of(t_dot(swish, do_all).reshape(zs, ys, part, width)))
    grad_gate = join_columns(t_dot(act_two, d_gate))
    grad_up = join_columns(t_dot(act_two, d_up))

    g_o = t_dot(mixed, d_branch)
    if paired:
        g_o = g_o.reshape(2, 2, depth, width)
        mine = lax.dynamic_index_in_dim(g_o, c, 1, keepdims=False)
        other = lax.dynamic_index_in_dim(g_o, 1 - c, 1, keepdims=False)
        other = swap(other.astype(BF), "c").astype(F32)
        both = jnp.stack([jnp.where(c == 0, mine, other), jnp.where(c == 0, other, mine)])
        grad_output = scatter_dp(blocks_of(both))
    else:
        g_full = lax.dynamic_update_slice(
            jnp.zeros((width, width), F32), g_o, (tp_index() * own_width, 0)
        )
        grad_output = lax.psum_scatter(g_full, AXES, scatter_dimension=0, tiled=True)
    d_mixed = dot_t(d_branch, w_o).astype(BF)
    d_mixed = d_mixed.reshape(buffers, cap, own_heads, HD).transpose(0, 2, 1, 3)
    d_probs = batched("bhqd,bkd->bhqk", d_mixed, v_low)
    d_v = batched("bhqk,bhqd->bkd", probs_low, d_mixed)
    d_v = jnp.concatenate([d_v[:mb] + d_value.astype(F32), d_v[mb:]], axis=0)
    d_logits = (probs * (d_probs - jnp.sum(probs * d_probs, axis=-1, keepdims=True))).astype(BF)
    d_q = batched("bhqk,bkd->bhqd", d_logits, k_rot) * scale
    d_k = batched("bhqk,bhqd->bkd", d_logits, q_rot) * scale
    d_k = jnp.concatenate([d_k[:mb] + d_key.astype(F32), d_k[mb:]], axis=0)
    d_q = rotate(d_q, cos_h, -sin_h).astype(BF).transpose(0, 2, 1, 3).reshape(rows, own_width)
    d_k = rotate(d_k, cosine, -sine).astype(BF).reshape(rows, HD)
    d_v = d_v.astype(BF).reshape(rows, HD)
    d_qkv = jnp.concatenate([d_q, d_k, d_v], axis=1)
    d_act_part = dot_t(d_qkv, w_qkv)
    d_act = scatter_tp(d_act_part)
    normed = xf * inverse_norm(xf)
    grad_gain_one = scatter_all(jnp.sum(d_act_part * normed, axis=0))

    g = scatter_dp(rows_of(t_dot(act, d_qkv)))
    g = exchange_tp(g.astype(BF)).astype(F32)
    g_q = g[:, :, :own_width]
    if paired:
        g_q = g_q.reshape(2, 2, 2, depth, 2, HD).transpose(3, 2, 0, 4, 1, 5)
    else:
        g_q = g_q.transpose(1, 0, 2)
    grad_query = g_q.reshape(depth, width)
    g_kv = jnp.sum(g[:, :, own_width:], axis=0)

    x_f = x_own.astype(F32)
    inverse_own = inverse_norm(x_f)
    normed_own = x_f * inverse_own
    scaled = d_act * gain_a
    d_inputs = d_hidden + inverse_own * (
        scaled - normed_own * jnp.mean(scaled * normed_own, axis=-1, keepdims=True)
    )
    return (
        output.reshape(mb, cap, width),
        k_rot[:mb],
        v_low[:mb],
        d_inputs.astype(BF).reshape(mb, cap, width),
        grad_gain_one,
        grad_query,
        g_kv[:, :HD],
        g_kv[:, HD:],
        grad_output,
        grad_gain_two,
        grad_gate,
        grad_up,
        grad_down,
    )


def solution(mesh):
    dp, fsdp = mesh.devices.shape
    grid = Mesh(mesh.devices.reshape(dp // 2, 2, fsdp // 4, 2, 2), AXES)
    rows = P(AXES)
    seq = P(None, AXES)
    return jax.shard_map(
        per_device,
        mesh=grid,
        in_specs=(seq, seq) + (rows,) * 9 + (seq,) * 3,
        out_specs=(seq,) * 4 + (rows,) * 9,
        check_vma=False,
    )
```
